256 devices in a mesh: term: 16 (over z, core), sector: 16 (over y, x).
Axes of the slice: x: 4, y: 4, z: 8, core: 2. Of those that a mesh axis runs over, the one named last changes fastest.
Arguments:
- wavefunction: bfloat16 [96, 256, 256], P('sector'), may hold values from -6 to 6
- left_env: bfloat16 [48, 96, 256, 256], P('term', 'sector')
- right_env: bfloat16 [48, 96, 256, 256], P('term', 'sector')
- source: int32 [48, 96], P('term'), may hold values from 0 to 95, as said below
- block_size: int32 [96, 2], P('sector'), may hold values from 32 to 256
Outputs:
- first_product: float32 [96, 256, 256], P('sector', 'term')
- second_product: float32 [96, 256, 256], P('sector', 'term')
The draws below stay inside these ranges and needn't reach their ends.
Inputs may be any that keep to these rules, and one draw needn't show every extreme that they name: Owner of sector s is s // 6. Among the 3 x 6 entries of source in one device's rows (one index of term) and columns (one index of sector), at most 2 name sectors of any one owner, and some owner is named exactly 2 times.
All inputs are finite; a program needn't handle non-finite values.
Results may differ from the reference program's by a relative error of at most 0.0037.
Values may be sent and summed in bfloat16 or wider, within the bound.
No kernel may reach another device: no remote copies, remote signals or barrier semaphores. Data moves between devices by JAX's collectives and lax.ppermute only.
A program may use at most 64 MiB of HBM per device.

```python
import math
import jax
import jax.numpy as jnp
from jax import lax

DL = 256
SEC_DEV = 6
B_DEV = 3
SECTORS = 96
BONDS = 48
CAP = 2


def environment(key, salt):
    base = jax.random.fold_in(key, salt)
    diagonal = jax.random.uniform(jax.random.fold_in(base, 1), (BONDS, SECTORS, DL), jnp.float32, 0.2, 1.2)
    noise = jax.random.normal(jax.random.fold_in(base, 2), (BONDS, SECTORS, DL, DL), jnp.float32)
    identity_table = jnp.eye(DL, dtype=jnp.float32)
    matrix = (noise * (0.6 / math.sqrt(DL)) + diagonal[..., None] * identity_table) / math.sqrt(BONDS)
    return matrix.astype(jnp.bfloat16)


def draw_left_env(key, part):
    return environment(key, 101)


def draw_right_env(key, part):
    return environment(key, 202)


def draw_source(key, part):
    term_groups = BONDS // B_DEV
    sector_groups = SECTORS // SEC_DEV
    item_count = B_DEV * SEC_DEV
    base = jax.random.fold_in(key, 303)

    def one_block(number):
        block_key = jax.random.fold_in(base, number)
        order = jax.random.permutation(jax.random.fold_in(block_key, 1), item_count)
        owners = jax.random.permutation(jax.random.fold_in(block_key, 2), sector_groups)
        owner_of = owners[order // CAP]
        local_slot = jax.random.randint(jax.random.fold_in(block_key, 3), (item_count,), 0, SEC_DEV)
        return (owner_of * SEC_DEV + local_slot).astype(jnp.int32)
    blocks = jax.vmap(one_block)(jnp.arange(term_groups * sector_groups, dtype=jnp.int32))
    blocks = blocks.reshape(term_groups, sector_groups, B_DEV, SEC_DEV).transpose(0, 2, 1, 3)
    return blocks.reshape(BONDS, SECTORS)


def plant(array, own_key, smallest, high):
    dims = array.shape
    spot = [jax.random.randint(jax.random.fold_in(own_key, axis), (), 0, dims[axis]) for axis in range(len(dims))]
    array = array.at[tuple(spot)].set(smallest)
    longest = dims.index(max(dims))
    spot[longest] = (spot[longest] + 1) % dims[longest]
    return array.at[tuple(spot)].set(high)


def block_scale(stream_key, shape, split, low, largest):
    level, own = 1.0, jax.random.fold_in(stream_key, 6)
    for axis_at, shards_of in split:
        steps = jnp.exp(jax.random.uniform(jax.random.fold_in(own, axis_at), (shards_of,), jnp.float32, low / len(split), largest / len(split)))
        level = level * jnp.repeat(steps, shape[axis_at] // shards_of).reshape([-1 if axis == axis_at else 1 for axis in range(len(shape))])
    return level


def centred(stream_key, dims, scale, bound, shards=(), kind=jnp.bfloat16):
    drawn = scale * jax.random.normal(stream_key, dims, jnp.float32)
    if shards:
        drawn = drawn * block_scale(stream_key, dims, shards, -0.22, 0.18)
    return jnp.clip(drawn, -bound, bound).astype(kind)


def setup_inputs(seed: int = 0) -> dict:
    arg_keys = jax.random.split(jax.random.key(seed), 6)
    return {
        "wavefunction": centred(arg_keys[0], (SECTORS, DL, DL), 1.0, 6.0, ((0, 16),)),
        "left_env": draw_left_env(jax.random.fold_in(arg_keys[5], 71), 0),
        "right_env": draw_right_env(jax.random.fold_in(arg_keys[5], 71), 0),
        "source": draw_source(jax.random.fold_in(arg_keys[5], 71), 0),
        "block_size": plant(jax.random.randint(arg_keys[4], (SECTORS, 2), DL // 8, DL + 1), jax.random.fold_in(arg_keys[4], 1), DL // 8, DL).astype(jnp.int32),
    }


epsilon = 1e-06

def block_mask(block_size, width):
    positions = jnp.arange(width, dtype=jnp.int32)
    row_keep = positions[None, :] < block_size[:, 0:1]
    column_keep = positions[None, :] < block_size[:, 1:2]
    return row_keep[:, :, None] & column_keep[:, None, :]

def apply_operator(vector, left_env, right_env, source, keep):
    masked = jnp.where(keep, vector, jnp.zeros_like(vector))

    def one_bond(summed, inputs):
        left_bond, right_bond, source_bond = inputs
        picked = jnp.take(masked, source_bond.astype(jnp.int32), axis=0)
        half_product = jnp.einsum('kij,kjl->kil', left_bond.astype(jnp.float32), picked.astype(jnp.float32)).astype(jnp.bfloat16)
        bond_term = jnp.einsum('kil,kml->kim', half_product.astype(jnp.float32), right_bond.astype(jnp.float32))
        return (summed + bond_term, None)
    initial = jnp.zeros(masked.shape, jnp.float32)
    summed, _ = lax.scan(one_bond, initial, (left_env, right_env, source))
    return (jnp.where(keep, summed, jnp.zeros_like(summed)), masked)

def reference(wavefunction, left_env, right_env, source, block_size):
    keep = block_mask(block_size, DL)
    first_product, masked = apply_operator(wavefunction, left_env, right_env, source, keep)
    masked_float = masked.astype(jnp.float32)
    margin = jnp.sum(masked_float * first_product)
    self_norm = jnp.sum(masked_float * masked_float)
    residual = first_product - margin / self_norm * masked_float
    spread = jnp.sum(residual * residual)
    next_vector = (residual * lax.rsqrt(spread / (SECTORS * DL * DL) + epsilon)).astype(jnp.bfloat16)
    second_product, _ = apply_operator(next_vector, left_env, right_env, source, keep)
    return (first_product, second_product)
```

```python
import functools

import jax
import jax.numpy as jnp
from jax import lax
from jax.experimental import pallas as pl
from jax.experimental.pallas import tpu as pltpu
from jax.sharding import PartitionSpec as P

epsilon = 1e-06
EXTRA = 16
F32 = jnp.float32
BF16 = jnp.bfloat16


def pieces_of(value):
    high = value.astype(BF16)
    rest = value - high.astype(F32)
    middle = rest.astype(BF16)
    low = (rest - middle.astype(F32)).astype(BF16)
    return [high, middle, low]


def joined(parts, at):
    return parts[:, at] + parts[:, at + 1] + parts[:, at + 2]


def ratio(above, below):
    live = below > 0
    return jnp.where(live, above / jnp.where(live, below, 1.0), 0.0)


def totals_of(extra):
    parts = extra.astype(F32)
    norms, margins, spreads = joined(parts, 0), joined(parts, 3), joined(parts, 6)
    norm = jnp.sum(norms, axis=0, keepdims=True)
    margin = jnp.sum(margins, axis=0, keepdims=True)
    own = ratio(margins, norms)
    shift = ratio(margin, norm) - own
    moved = spreads - 2.0 * shift * (margins - own * norms) + shift * shift * norms
    return norm, margin, jnp.sum(moved, axis=0, keepdims=True)


def rows_of_pieces(values, width):
    rows = [row for value in values for row in pieces_of(value)]
    rows = [jnp.broadcast_to(row, (1, width)).astype(F32) for row in rows]
    rows.append(jnp.zeros((EXTRA - len(rows), width), F32))
    return jnp.concatenate(rows, axis=0).astype(BF16)


def keep_of(rows, columns, shape, first_row=0):
    row = lax.broadcasted_iota(jnp.int32, shape, 0) + first_row
    column = lax.broadcasted_iota(jnp.int32, shape, 1)
    return (row < rows) & (column < columns)


def pack_masked_kernel(slots, sizes, wave, out, masked):
    peer = pl.program_id(0)
    count, width = wave.shape[0], wave.shape[1]

    @pl.when(peer == 0)
    def _():
        for k in range(count):
            keep = keep_of(sizes[2 * k], sizes[2 * k + 1], (width, width))
            masked[k] = jnp.where(keep, wave[k].astype(F32), 0.0).astype(BF16)

    capacity = out.shape[1] // width
    for c in range(capacity):
        out[0, pl.ds(c * width, width), :] = masked[slots[peer * capacity + c]]


def pack_masked(slots, sizes, wave, peers, capacity):
    count, width, _ = wave.shape
    return pl.pallas_call(
        pack_masked_kernel,
        grid_spec=pltpu.PrefetchScalarGridSpec(
            num_scalar_prefetch=2,
            grid=(peers,),
            in_specs=[pl.BlockSpec((count, width, width), lambda p, *_: (0, 0, 0))],
            out_specs=pl.BlockSpec((1, capacity * width, width), lambda p, *_: (p, 0, 0)),
            scratch_shapes=[pltpu.VMEM((count, width, width), BF16)],
        ),
        out_shape=jax.ShapeDtypeStruct((peers, capacity * width, width), BF16),
        name="pack_masked",
    )(slots, sizes, wave)


def pack_first_kernel(slots, gathered, out):
    peer = pl.program_id(0)
    terms, lines, width = gathered.shape
    rows = width // terms
    capacity = (out.shape[1] - EXTRA) // width
    for c in range(capacity):
        slot = slots[peer * capacity + c]
        start = pl.multiple_of(slot * rows, rows)
        block = gathered[:, pl.ds(start, rows), :]
        out[0, pl.ds(c * width, width), :] = block.reshape(width, width)
    norm, margin, spread = totals_of(gathered[:, pl.ds(lines - EXTRA, EXTRA), :])
    out[0, pl.ds(capacity * width, EXTRA), :] = rows_of_pieces((norm, margin, spread), width)


def pack_first(slots, gathered, peers, capacity):
    terms, lines, width = gathered.shape
    out_lines = capacity * width + EXTRA
    return pl.pallas_call(
        pack_first_kernel,
        grid_spec=pltpu.PrefetchScalarGridSpec(
            num_scalar_prefetch=1,
            grid=(peers,),
            in_specs=[pl.BlockSpec((terms, lines, width), lambda p, *_: (0, 0, 0))],
            out_specs=pl.BlockSpec((1, out_lines, width), lambda p, *_: (p, 0, 0)),
        ),
        out_shape=jax.ShapeDtypeStruct((peers, out_lines, width), BF16),
        name="pack_first",
    )(slots, gathered)


def bond_sum(vectors, left, right):
    total = None
    for b, vector in enumerate(vectors):
        half = jnp.dot(left[b, 0], vector, preferred_element_type=F32).astype(BF16)
        term = lax.dot_general(half, right[b, 0], (((1,), (1,)), ((), ())), preferred_element_type=F32)
        total = term if total is None else total + term
    return total


def store_partial(total, sizes, out):
    k = pl.program_id(0)
    keep = keep_of(sizes[2 * k], sizes[2 * k + 1], total.shape)
    total = jnp.where(keep, total, 0.0).astype(BF16)
    out[:, 0] = total.reshape(out.shape[0], out.shape[2], out.shape[3])


def first_kernel(bonds, owners, ranks, sizes, *refs):
    left, right, out = refs[bonds:]
    store_partial(bond_sum([r[0] for r in refs[:bonds]], left, right), sizes, out)


def second_kernel(bonds, count, owners, ranks, sizes, *refs):
    waves, firsts = refs[:bonds], refs[bonds : 2 * bonds]
    extra, left, right, out = refs[2 * bonds :]
    norm, margin, spread = totals_of(extra[...])
    scale = lax.rsqrt(jnp.maximum(spread, 0.0) / count + epsilon)
    share = margin / norm
    vectors = []
    for wave, first in zip(waves, firsts):
        residual = first[0].astype(F32) - share * wave[0].astype(F32)
        vectors.append((residual * scale).astype(BF16))
    store_partial(bond_sum(vectors, left, right), sizes, out)


def product(owners, ranks, sizes, arrived, left, right, terms, total_count=None):
    bonds, count, width, _ = left.shape

    def picked(b):
        return pl.BlockSpec((1, width, width), lambda k, own, rank, *_: (own[b * count + k], rank[b * count + k], 0))

    env = pl.BlockSpec((bonds, 1, width, width), lambda k, *_: (0, k, 0, 0))
    operands, specs = [], []
    for array in arrived:
        operands += [array] * bonds
        specs += [picked(b) for b in range(bonds)]
    if total_count is None:
        kernel = functools.partial(first_kernel, bonds)
    else:
        kernel = functools.partial(second_kernel, bonds, total_count)
        lines = arrived[1].shape[1]
        operands.append(arrived[1])
        specs.append(pl.BlockSpec((arrived[1].shape[0], EXTRA, width), lambda k, *_: (0, lines // EXTRA - 1, 0)))
    return pl.pallas_call(
        kernel,
        grid_spec=pltpu.PrefetchScalarGridSpec(
            num_scalar_prefetch=3,
            grid=(count,),
            in_specs=specs + [env, env],
            out_specs=pl.BlockSpec((terms, 1, width // terms, width), lambda k, *_: (0, k, 0, 0)),
        ),
        out_shape=jax.ShapeDtypeStruct((terms, count, width // terms, width), BF16),
        name="product",
    )(owners, ranks, sizes, *operands, left, right)


def middle_kernel(term, sizes, arrived, wave, first_out, message):
    terms, count, rows, width = arrived.shape
    summed = arrived[0].astype(F32)
    for t in range(1, terms):
        summed = summed + arrived[t].astype(F32)
    first_out[...] = summed
    kept = []
    for k in range(count):
        keep = keep_of(sizes[2 * k], sizes[2 * k + 1], (rows, width), term[0] * rows)
        kept.append(jnp.where(keep, wave[k].astype(F32), 0.0)[None])
    masked = jnp.concatenate(kept, axis=0)

    def whole(values):
        return jnp.sum(jnp.sum(jnp.sum(values, axis=0), axis=0, keepdims=True), axis=1, keepdims=True)

    margin = whole(masked * summed)
    norm = whole(masked * masked)
    residual = summed - ratio(margin, norm)[None] * masked
    spread = whole(residual * residual)
    extra = rows_of_pieces((norm, margin, spread), width)
    lines = summed.astype(BF16).reshape(count * rows, width)
    for t in range(terms):
        message[t, pl.ds(0, count * rows), :] = lines
        message[t, pl.ds(count * rows, EXTRA), :] = extra


def middle(term, sizes, arrived, wave):
    terms, count, rows, width = arrived.shape
    lines = count * rows + EXTRA
    return pl.pallas_call(
        middle_kernel,
        grid_spec=pltpu.PrefetchScalarGridSpec(
            num_scalar_prefetch=2,
            grid=(1,),
            in_specs=[
                pl.BlockSpec((terms, count, rows, width), lambda i, *_: (0, 0, 0, 0)),
                pl.BlockSpec((count, rows, width), lambda i, t, *_: (0, t[0], 0)),
            ],
            out_specs=[
                pl.BlockSpec((count, rows, width), lambda i, *_: (0, 0, 0)),
                pl.BlockSpec((terms, lines, width), lambda i, *_: (0, 0, 0)),
            ],
        ),
        out_shape=[
            jax.ShapeDtypeStruct((count, rows, width), F32),
            jax.ShapeDtypeStruct((terms, lines, width), BF16),
        ],
        name="middle",
    )(term, sizes, arrived, wave)


def exchanged(array, axis):
    return lax.all_to_all(array, axis, split_axis=0, concat_axis=0, tiled=True)


def routes(source, count, capacity):
    peers = lax.axis_size("sector")
    me = lax.axis_index("sector")
    bonds = source.shape[0]
    needs = source.reshape(bonds, peers, count).transpose(1, 0, 2).reshape(peers, bonds * count)
    first_mine = me * count
    local = needs - first_mine
    here = (local >= 0) & (local < count)
    items = bonds * count
    earlier = jnp.arange(items)[:, None] < jnp.arange(items)[None, :]
    rank = jnp.sum(here[:, :, None] & earlier[None], axis=1)
    chosen = here[:, None, :] & (rank[:, None, :] == jnp.arange(capacity)[None, :, None])
    slots = jnp.sum(jnp.where(chosen, local[:, None, :], 0), axis=2).reshape(-1)
    mine = lax.dynamic_index_in_dim(needs, me, 0, keepdims=False)
    owners = lax.div(mine, jnp.int32(count))
    ranks = jnp.sum((owners[:, None] == owners[None, :]) & earlier, axis=0)
    return slots.astype(jnp.int32), owners, ranks.astype(jnp.int32)


def body(wavefunction, left_env, right_env, source, block_size):
    count, width, _ = wavefunction.shape
    peers, terms = lax.axis_size("sector"), lax.axis_size("term")
    capacity = max(2, left_env.shape[0] * count // peers + 1)
    term = lax.axis_index("term").reshape(1).astype(jnp.int32)
    sizes = block_size.reshape(-1)
    slots, owners, ranks = routes(source, count, capacity)
    waves = exchanged(pack_masked(slots, sizes, wavefunction, peers, capacity), "sector")
    partial = product(owners, ranks, sizes, [waves], left_env, right_env, terms)
    first_product, message = middle(term, sizes, exchanged(partial, "term"), wavefunction)
    gathered = exchanged(message, "term")
    firsts = exchanged(pack_first(slots, gathered, peers, capacity), "sector")
    total_count = peers * count * width * width
    partial = product(owners, ranks, sizes, [waves, firsts], left_env, right_env, terms, total_count)
    second_product = jnp.sum(exchanged(partial, "term").astype(F32), axis=0)
    return (first_product, second_product)


def solution(mesh):
    placed = (
        P("sector", None, None),
        P("term", "sector", None, None),
        P("term", "sector", None, None),
        P("term", None),
        P("sector", None),
    )
    return jax.shard_map(
        body,
        mesh=mesh,
        in_specs=placed,
        out_specs=(P("sector", "term", None), P("sector", "term", None)),
        check_vma=False,
    )
```

```python
import functools

import jax
import jax.numpy as jnp
from jax import lax
from jax.experimental import pallas as pl
from jax.experimental.pallas import tpu as pltpu
from jax.sharding import Mesh, PartitionSpec as P

epsilon = 1e-06
AXES = ("z", "core", "y", "x")
GRID = (8, 2, 4, 4)
RING = 4
EXTRA = 16
TAIL = 8
F32 = jnp.float32
BF16 = jnp.bfloat16


def pieces_of(value, count=3):
    pieces, rest = [], value
    for _ in range(count):
        piece = rest.astype(BF16)
        pieces.append(piece.astype(F32))
        rest = rest - pieces[-1]
    return pieces


def ratio(above, below):
    live = below > 0
    return jnp.where(live, above / jnp.where(live, below, 1.0), 0.0)


def totals_of(extra, last):
    parts = extra.astype(F32)
    norms = parts[:, 0] + parts[:, 1] + parts[:, 2]
    margins = parts[:, 3] + parts[:, 4] + parts[:, 5]
    spreads = sum(parts[:, 7 + i] for i in range(last - 1)) + parts[:, 6]
    norm = jnp.sum(norms, axis=0, keepdims=True)
    margin = jnp.sum(margins, axis=0, keepdims=True)
    own = ratio(margins, norms)
    shift = ratio(margin, norm) - own
    moved = spreads - 2.0 * shift * (margins - own * norms) + shift * shift * norms
    return norm, margin, jnp.sum(moved, axis=0, keepdims=True)


def rows_of_pieces(norm, margin, spread, last, lines, lanes):
    rows = pieces_of(norm) + pieces_of(margin) + pieces_of(spread, last)
    rows = [jnp.broadcast_to(row, (1, lanes)) for row in rows]
    if lines > len(rows):
        rows.append(jnp.zeros((lines - len(rows), lanes), F32))
    return jnp.concatenate(rows, axis=0).astype(BF16)


def keep_of(rows, columns, shape, first_row=0, first_column=0):
    row = lax.broadcasted_iota(jnp.int32, shape, 0) + first_row
    column = lax.broadcasted_iota(jnp.int32, shape, 1) + first_column
    return (row < rows) & (column < columns)


def masked_kernel(place, sizes, wave, out):
    count, width, lanes = wave.shape
    for k in range(count):
        keep = keep_of(sizes[k, 0], sizes[k, 1], (width, lanes), 0, place[1] * lanes)
        out[pl.ds(k * width, width), :] = jnp.where(keep, wave[k].astype(F32), 0.0).astype(BF16)


def masked_half(place, sizes, wave):
    count, width, _ = wave.shape
    lanes = width // 2
    return pl.pallas_call(
        masked_kernel,
        grid_spec=pltpu.PrefetchScalarGridSpec(
            num_scalar_prefetch=2,
            grid=(1,),
            in_specs=[pl.BlockSpec((count, width, lanes), lambda i, place, *_: (0, 0, place[1]))],
            out_specs=pl.BlockSpec((count * width, lanes), lambda i, *_: (0, 0)),
        ),
        out_shape=jax.ShapeDtypeStruct((count * width, lanes), BF16),
        name="masked_half",
    )(place, sizes, wave)


def middle_kernel(place, sizes, arrived, wave, first_out, message):
    peers, count, rows, lanes = arrived.shape
    summed = arrived[0].astype(F32)
    for t in range(1, peers):
        summed = summed + arrived[t].astype(F32)
    first_out[...] = summed
    kept = []
    for k in range(count):
        keep = keep_of(sizes[k, 0], sizes[k, 1], (rows, lanes), place[0] * rows, place[1] * lanes)
        kept.append(jnp.where(keep, wave[k].astype(F32), 0.0)[None])
    masked = jnp.concatenate(kept, axis=0)

    def whole(values):
        return jnp.sum(jnp.sum(jnp.sum(values, axis=0), axis=0, keepdims=True), axis=1, keepdims=True)

    margin = whole(masked * summed)
    norm = whole(masked * masked)
    residual = summed - ratio(margin, norm)[None] * masked
    spread = whole(residual * residual)
    message[pl.ds(0, count * rows), :] = summed.astype(BF16).reshape(count * rows, lanes)
    message[pl.ds(count * rows, EXTRA), :] = rows_of_pieces(norm, margin, spread, 3, EXTRA, lanes)


def middle(place, sizes, arrived, wave):
    peers, count, rows, lanes = arrived.shape
    lines = count * rows + EXTRA
    return pl.pallas_call(
        middle_kernel,
        grid_spec=pltpu.PrefetchScalarGridSpec(
            num_scalar_prefetch=2,
            grid=(1,),
            in_specs=[
                pl.BlockSpec((peers, count, rows, lanes), lambda i, *_: (0, 0, 0, 0)),
                pl.BlockSpec((count, rows, lanes), lambda i, place, *_: (0, place[0], place[1])),
            ],
            out_specs=[
                pl.BlockSpec((count, rows, lanes), lambda i, *_: (0, 0, 0)),
                pl.BlockSpec((lines, lanes), lambda i, *_: (0, 0)),
            ],
        ),
        out_shape=[
            jax.ShapeDtypeStruct((count, rows, lanes), F32),
            jax.ShapeDtypeStruct((lines, lanes), BF16),
        ],
        name="middle",
    )(place, sizes, arrived, wave)


def collect_kernel(count, place, gathered, out):
    terms, lines, lanes = gathered.shape
    rows = (lines - EXTRA) // count
    planes = terms // 2
    width = planes * rows
    for z in range(planes):
        part = gathered[2 * z + place[1]]
        for k in range(count):
            out[pl.ds(k * width + z * rows, rows), :] = part[k * rows : (k + 1) * rows]
    norm, margin, spread = totals_of(gathered[:, pl.ds(count * rows, EXTRA), :], 3)
    out[pl.ds(count * width, TAIL), :] = rows_of_pieces(norm, margin, spread, 2, TAIL, lanes)


def collect(place, gathered, count):
    terms, lines, lanes = gathered.shape
    out_lines = terms // 2 * (lines - EXTRA) + TAIL
    return pl.pallas_call(
        functools.partial(collect_kernel, count),
        grid_spec=pltpu.PrefetchScalarGridSpec(
            num_scalar_prefetch=1,
            grid=(1,),
            in_specs=[pl.BlockSpec((terms, lines, lanes), lambda i, *_: (0, 0, 0))],
            out_specs=pl.BlockSpec((out_lines, lanes), lambda i, *_: (0, 0)),
        ),
        out_shape=jax.ShapeDtypeStruct((out_lines, lanes), BF16),
        name="collect",
    )(place, gathered)


def plane_pairs(inner, distance):
    pairs = []
    for core in range(2):
        for y in range(RING):
            for x in range(RING):
                if (core == 0) == inner:
                    to = (y, (x + distance) % RING)
                else:
                    to = ((y + distance) % RING, x)
                pairs.append(((core * RING + y) * RING + x, (core * RING + to[0]) * RING + to[1]))
    return pairs


def moved(array, inner, distance):
    return lax.ppermute(array, ("core", "y", "x"), plane_pairs(inner, distance))


def swapped(array):
    return lax.ppermute(array, "core", [(0, 1), (1, 0)])


def plane_gather(own):
    line = jnp.concatenate([own, moved(own, True, 1), moved(own, True, -1), moved(own, True, 2)], axis=0)
    half = line.shape[0] // 2
    low, high = line[:half], line[half:]
    below_low, above_high = moved(low, False, 1), moved(high, False, -1)
    below_high, above_low = moved(high, False, 1), moved(low, False, -1)
    far_low, far_high = moved(below_low, False, 1), moved(above_high, False, -1)
    return [line, above_low, above_high, far_low, far_high, below_low, below_high]


def places_of(source, lines, count, width):
    owner = lax.div(source, jnp.int32(count))
    local = source - owner * count
    y_off = (lax.div(owner, jnp.int32(RING)) - lax.axis_index("y")) & (RING - 1)
    x_off = (owner - lax.axis_index("x")) & (RING - 1)
    first = lax.axis_index("core") == 0
    inner = jnp.where(first, x_off, y_off)
    outer = jnp.where(first, y_off, x_off)
    order = jnp.where(inner == 0, 0, jnp.where(inner == 3, 1, inner + 1))
    high = order >> 1
    piece = jnp.where(outer == 0, 0, 2 * outer - 1 + high)
    slot = jnp.where(outer == 0, order, order & 1)
    return piece, slot * lines + local * width


def product_kernel(second, count_all, lines, piece, start, sizes, place, *refs):
    sources, refs = refs[:7], refs[7:]
    if second:
        waves, refs = refs[0], refs[1:]
    left, left_other, right, right_other = refs[:4]
    if second:
        mine, theirs, buffer, arrived, stats, stats_arrived = refs[4:]
    else:
        mine, theirs, picked, buffer, arrived = refs[4:]
    k = pl.program_id(0)
    items, width, lanes = buffer.shape
    bonds = left.shape[0] + left_other.shape[0]

    @pl.when(k == 0)
    def _():
        def begin(j, carry):
            line = pl.multiple_of(start[j], 8)
            for n, ref in enumerate(sources):

                @pl.when(piece[j] == n)
                def _():
                    pltpu.make_async_copy(ref.at[pl.ds(line, width), :], buffer.at[j], arrived.at[j]).start()

            return carry

        lax.fori_loop(0, items, begin, 0)
        if second:
            copies = []
            for n, ref in enumerate(sources):
                for slot in range(4 if n == 0 else 2):
                    at = len(copies)
                    tail = pl.ds(slot * lines + lines - TAIL, TAIL)
                    copies.append(pltpu.make_async_copy(ref.at[tail, :], stats.at[at], stats_arrived.at[at]))
            for copy in copies:
                copy.start()
            for copy in copies:
                copy.wait()

    if second:
        norm, margin, spread = totals_of(stats[...], 2)
        scale = lax.rsqrt(jnp.maximum(spread, 0.0) / count_all + epsilon)
        share = margin / norm
    halves, rights = [], []
    for b in range(bonds):
        j = k * bonds + b
        pltpu.make_async_copy(sources[0].at[pl.ds(0, width), :], buffer.at[j], arrived.at[j]).wait()
        vector = buffer[j]
        if second:
            residual = vector.astype(F32) - share * waves[b].astype(F32)
            vector = (residual * scale).astype(BF16)
        else:
            picked[b] = vector
        at = b % left.shape[0]
        env, other = (left, right) if b < left.shape[0] else (left_other, right_other)
        halves.append(jnp.dot(env[at, 0], vector, preferred_element_type=F32).astype(BF16))
        rights.append(other[at, 0])
    total = lax.dot_general(
        jnp.concatenate(halves, axis=1),
        jnp.concatenate(rights, axis=1),
        (((1,), (1,)), ((), ())),
        preferred_element_type=F32,
    )
    total = jnp.where(keep_of(sizes[k, 0], sizes[k, 1], total.shape), total, 0.0)
    planes, _, rows, columns = mine.shape
    if second:
        parts = total.reshape(planes, 2, rows, columns)
        low, high = parts[:, 0], parts[:, 1]
    else:
        parts = total.reshape(planes, rows, 2 * columns)
        low, high = parts[:, :, :columns], parts[:, :, columns:]

    @pl.when(place[1] == 0)
    def _():
        mine[:, 0] = low
        theirs[:, 0] = high.astype(BF16)

    @pl.when(place[1] == 1)
    def _():
        mine[:, 0] = high
        theirs[:, 0] = low.astype(BF16)


def product(piece, start, sizes, place, sources, env, waves=None, count_all=None):
    left, left_other, right, right_other = env
    own, count, width, _ = left.shape
    bonds, lanes = 2 * own, width // 2
    items = count * bonds
    second = waves is not None
    lines = sources[0].shape[0] // 4
    planes = GRID[0]
    rows, columns = (width // planes // 2, width) if second else (width // planes, lanes)
    whole = pl.BlockSpec((own, 1, width, width), lambda k, *_: (0, k, 0, 0))
    group = pl.BlockSpec((bonds, width, lanes), lambda k, *_: (k, 0, 0))
    result = pl.BlockSpec((planes, 1, rows, columns), lambda k, *_: (0, k, 0, 0))
    in_specs = [pl.BlockSpec(memory_space=pl.ANY)] * len(sources) + ([group] if second else [])
    in_specs += [whole, whole]
    in_specs.append(pl.BlockSpec((own, 1, width, lanes), lambda k, p, s, z, place: (0, k, 0, place[1])))
    in_specs.append(pl.BlockSpec((own, 1, width, lanes), lambda k, *_: (0, k, 0, 0)))
    shape = (planes, count, rows, columns)
    out_shape = [jax.ShapeDtypeStruct(shape, F32), jax.ShapeDtypeStruct(shape, BF16)]
    out_specs = [result, result]
    scratch = [pltpu.VMEM((items, width, lanes), BF16), pltpu.SemaphoreType.DMA((items,))]
    if second:
        peers = RING * RING
        scratch += [pltpu.VMEM((peers, TAIL, lanes), BF16), pltpu.SemaphoreType.DMA((peers,))]
    else:
        out_shape.append(jax.ShapeDtypeStruct((items, width, lanes), BF16))
        out_specs.append(group)
    operands = list(sources) + ([waves] if second else []) + [left, left_other, right, right_other]
    return pl.pallas_call(
        functools.partial(product_kernel, second, count_all, lines),
        grid_spec=pltpu.PrefetchScalarGridSpec(
            num_scalar_prefetch=4,
            grid=(count,),
            in_specs=in_specs,
            out_specs=out_specs,
            scratch_shapes=scratch,
        ),
        out_shape=out_shape,
        name="product",
    )(piece, start, sizes, place, *operands)


def along_z(mine, theirs):
    both = (mine + swapped(theirs).astype(F32)).astype(BF16)
    return lax.all_to_all(both, "z", split_axis=0, concat_axis=0, tiled=True)


def body(wavefunction, left_env, right_env, source, block_size):
    count, width, _ = wavefunction.shape
    lanes = width // 2
    z, core = lax.axis_index("z"), lax.axis_index("core")
    sector = lax.axis_index("y") * RING + lax.axis_index("x")
    place = jnp.stack([z, core]).astype(jnp.int32)
    waves = plane_gather(masked_half(place, block_size, wavefunction))

    own_source = lax.dynamic_slice_in_dim(source, sector * count, count, 1)
    needs = jnp.concatenate([own_source, swapped(own_source)], axis=0).T.reshape(-1)
    left_other = swapped(left_env)
    right_other = swapped(lax.dynamic_slice_in_dim(right_env, (1 - core) * lanes, lanes, 3))
    env = (left_env, left_other, right_env, right_other)

    piece, start = places_of(needs, count * width, count, width)
    mine, theirs, picked = product(piece, start, block_size, place, waves, env)
    first, message = middle(place, block_size, along_z(mine, theirs), wavefunction)

    gathered = lax.all_gather(message, ("z", "core"), axis=0, tiled=False)
    firsts = plane_gather(collect(place, gathered, count))
    rows = width // GRID[0] // 2
    kept = lax.dynamic_slice_in_dim(first, core * rows, rows, 1)
    given = swapped(lax.dynamic_slice_in_dim(first, (1 - core) * rows, rows, 1))
    low, high = jnp.where(core == 0, kept, given), jnp.where(core == 0, given, kept)
    first_product = jnp.concatenate([low, high], axis=2)

    piece, start = places_of(needs, count * width + TAIL, count, width)
    count_all = RING * RING * count * width * width
    mine, theirs = product(piece, start, block_size, place, firsts, env, picked, count_all)
    second_product = jnp.sum(along_z(mine, theirs).astype(F32), axis=0)
    return (first_product, second_product)


def solution(mesh):
    chips = Mesh(mesh.devices.reshape(GRID), AXES)
    term, sector = ("z", "core"), ("y", "x")
    placed = (
        P(sector, None, None),
        P(term, sector, None, None),
        P(term, sector, None, None),
        P(term, None),
        P(sector, None),
    )
    return jax.shard_map(
        body,
        mesh=chips,
        in_specs=placed,
        out_specs=(P(sector, term, None), P(sector, term, None)),
        check_vma=False,
    )
```

```python
import functools

import jax
import jax.numpy as jnp
from jax import lax
from jax.experimental import pallas as pl
from jax.experimental.pallas import tpu as pltpu
from jax.sharding import Mesh, PartitionSpec as P

epsilon = 1e-06
AXES = ("z", "core", "y", "x")
GRID = (8, 2, 4, 4)
RING = 4
EXTRA = 16
F32 = jnp.float32
BF16 = jnp.bfloat16


def pieces_of(value):
    pieces, rest = [], value
    for _ in range(3):
        piece = rest.astype(BF16)
        pieces.append(piece.astype(F32))
        rest = rest - pieces[-1]
    return pieces


def ratio(above, below):
    live = below > 0
    return jnp.where(live, above / jnp.where(live, below, 1.0), 0.0)


def totals_of(extra):
    parts = extra.astype(F32)
    norms = parts[:, 0] + parts[:, 1] + parts[:, 2]
    margins = parts[:, 3] + parts[:, 4] + parts[:, 5]
    spreads = parts[:, 6] + parts[:, 7] + parts[:, 8]
    norm = jnp.sum(norms, axis=0, keepdims=True)
    margin = jnp.sum(margins, axis=0, keepdims=True)
    own = ratio(margins, norms)
    shift = ratio(margin, norm) - own
    moved = spreads - 2.0 * shift * (margins - own * norms) + shift * shift * norms
    return norm, margin, jnp.sum(moved, axis=0, keepdims=True)


def rows_of_pieces(values, lanes):
    rows = [jnp.broadcast_to(row, (1, lanes)) for value in values for row in pieces_of(value)]
    rows.append(jnp.zeros((EXTRA - len(rows), lanes), F32))
    return jnp.concatenate(rows, axis=0).astype(BF16)


def keep_of(rows, columns, shape, first_row=0, first_column=0):
    row = lax.broadcasted_iota(jnp.int32, shape, 0) + first_row
    column = lax.broadcasted_iota(jnp.int32, shape, 1) + first_column
    return (row < rows) & (column < columns)


def masked_half(core, sizes, wave):
    count, width, _ = wave.shape
    lanes = width // 2
    part = lax.dynamic_slice_in_dim(wave, core * lanes, lanes, 2)
    row = lax.broadcasted_iota(jnp.int32, part.shape, 1)
    column = lax.broadcasted_iota(jnp.int32, part.shape, 2) + core * lanes
    keep = (row < sizes[:, 0][:, None, None]) & (column < sizes[:, 1][:, None, None])
    return jnp.where(keep, part, jnp.zeros_like(part)).reshape(count * width, lanes)


def middle_kernel(place, sizes, arrived, wave, first_out, message):
    peers, count, rows, lanes = arrived.shape
    summed = arrived[0].astype(F32)
    for t in range(1, peers):
        summed = summed + arrived[t].astype(F32)
    first_out[...] = summed
    kept = []
    for k in range(count):
        keep = keep_of(sizes[k, 0], sizes[k, 1], (rows, lanes), place[0] * rows, place[1] * lanes)
        kept.append(jnp.where(keep, wave[k].astype(F32), 0.0)[None])
    masked = jnp.concatenate(kept, axis=0)

    def whole(values):
        return jnp.sum(jnp.sum(jnp.sum(values, axis=0), axis=0, keepdims=True), axis=1, keepdims=True)

    margin = whole(masked * summed)
    norm = whole(masked * masked)
    residual = summed - ratio(margin, norm)[None] * masked
    spread = whole(residual * residual)
    message[pl.ds(0, count * rows), :] = summed.astype(BF16).reshape(count * rows, lanes)
    message[pl.ds(count * rows, EXTRA), :] = rows_of_pieces((norm, margin, spread), lanes)


def middle(place, sizes, arrived, wave):
    peers, count, rows, lanes = arrived.shape
    lines = count * rows + EXTRA
    return pl.pallas_call(
        middle_kernel,
        grid_spec=pltpu.PrefetchScalarGridSpec(
            num_scalar_prefetch=2,
            grid=(1,),
            in_specs=[
                pl.BlockSpec((peers, count, rows, lanes), lambda i, *_: (0, 0, 0, 0)),
                pl.BlockSpec((count, rows, lanes), lambda i, place, *_: (0, place[0], place[1])),
            ],
            out_specs=[
                pl.BlockSpec((count, rows, lanes), lambda i, *_: (0, 0, 0)),
                pl.BlockSpec((lines, lanes), lambda i, *_: (0, 0)),
            ],
        ),
        out_shape=[
            jax.ShapeDtypeStruct((count, rows, lanes), F32),
            jax.ShapeDtypeStruct((lines, lanes), BF16),
        ],
        compiler_params=pltpu.CompilerParams(vmem_limit_bytes=8 << 20),
        name="middle",
    )(place, sizes, arrived, wave)


def collect_kernel(count, place, gathered, out):
    terms, lines, lanes = gathered.shape
    rows = (lines - EXTRA) // count
    planes = terms // 2
    width = planes * rows
    for z in range(planes):
        part = gathered[2 * z + place[1]]
        for k in range(count):
            out[pl.ds(k * width + z * rows, rows), :] = part[k * rows : (k + 1) * rows]
    totals = totals_of(gathered[:, pl.ds(count * rows, EXTRA), :])
    out[pl.ds(count * width, EXTRA), :] = rows_of_pieces(totals, lanes)


def collect(place, gathered, count):
    terms, lines, lanes = gathered.shape
    out_lines = terms // 2 * (lines - EXTRA) + EXTRA
    return pl.pallas_call(
        functools.partial(collect_kernel, count),
        grid_spec=pltpu.PrefetchScalarGridSpec(
            num_scalar_prefetch=1,
            grid=(1,),
            in_specs=[pl.BlockSpec((terms, lines, lanes), lambda i, *_: (0, 0, 0))],
            out_specs=pl.BlockSpec((out_lines, lanes), lambda i, *_: (0, 0)),
        ),
        out_shape=jax.ShapeDtypeStruct((out_lines, lanes), BF16),
        compiler_params=pltpu.CompilerParams(vmem_limit_bytes=8 << 20),
        name="collect",
    )(place, gathered)


def plane_pairs(inner, distance):
    pairs = []
    for core in range(2):
        for y in range(RING):
            for x in range(RING):
                if (core == 0) == inner:
                    to = (y, (x + distance) % RING)
                else:
                    to = ((y + distance) % RING, x)
                pairs.append(((core * RING + y) * RING + x, (core * RING + to[0]) * RING + to[1]))
    return pairs


def moved(array, inner, distance):
    return lax.ppermute(array, ("core", "y", "x"), plane_pairs(inner, distance))


def swapped(array):
    return lax.ppermute(array, "core", [(0, 1), (1, 0)])


def plane_gather(own):
    low = jnp.concatenate([own, moved(own, True, 1)], axis=0)
    high = jnp.concatenate([moved(own, True, -1), moved(own, True, 2)], axis=0)
    below_low, above_high = moved(low, False, 1), moved(high, False, -1)
    below_high, above_low = moved(high, False, 1), moved(low, False, -1)
    far_low, far_high = moved(below_low, False, 1), moved(above_high, False, -1)
    return [low, high, above_low, above_high, far_low, far_high, below_low, below_high]


def places_of(source, lines, count, width):
    owner = lax.div(source, jnp.int32(count))
    local = source - owner * count
    y_off = (lax.div(owner, jnp.int32(RING)) - lax.axis_index("y")) & (RING - 1)
    x_off = (owner - lax.axis_index("x")) & (RING - 1)
    first = lax.axis_index("core") == 0
    inner = jnp.where(first, x_off, y_off)
    outer = jnp.where(first, y_off, x_off)
    order = jnp.where(inner == 0, 0, jnp.where(inner == 3, 1, inner + 1))
    return 2 * outer + (order >> 1), (order & 1) * lines + local * width


def product_kernel(second, count_all, lines, piece, start, sizes, place, *refs):
    sources, refs = refs[:8], refs[8:]
    if second:
        waves, left, left_other, right, right_other, mine, theirs, vectors = refs
    else:
        left, left_other, right, right_other, mine, theirs, vectors = refs
    own, count, width, _ = left.shape
    lanes = width // 2
    bonds = 2 * own
    core = place[1]
    columns = pl.ds(pl.multiple_of(core * lanes, lanes), lanes)
    if second:
        tails = [ref[pl.ds(slot * lines + lines - EXTRA, EXTRA), :][None] for ref in sources for slot in range(2)]
        norm, margin, spread = totals_of(jnp.concatenate(tails, axis=0))
        scale = lax.rsqrt(jnp.maximum(spread, 0.0) / count_all + epsilon)
        share = margin / norm

    def pick(j, carry):
        line = pl.multiple_of(start[j], EXTRA)
        for n, ref in enumerate(sources):

            @pl.when(piece[j] == n)
            def _():
                vectors[j] = ref[pl.ds(line, width), :]

        return carry

    def one(k, carry):
        halves, rights = [], []
        for b in range(bonds):
            vector = vectors[k * bonds + b]
            if second:
                residual = vector.astype(F32) - share * waves[k * bonds + b].astype(F32)
                vector = (residual * scale).astype(BF16)
            at = b % own
            env = left if b < own else left_other
            halves.append(jnp.dot(env[at, k], vector, preferred_element_type=F32).astype(BF16))
            rights.append(right[at, k, :, columns] if b < own else right_other[at, k])
        total = lax.dot_general(
            jnp.concatenate(halves, axis=1),
            jnp.concatenate(rights, axis=1),
            (((1,), (1,)), ((), ())),
            preferred_element_type=F32,
        )
        total = jnp.where(keep_of(sizes[k, 0], sizes[k, 1], total.shape), total, 0.0)
        planes, _, rows, wide = mine.shape
        if second:
            parts = total.reshape(planes, 2, rows, wide)
            low, high = parts[:, 0], parts[:, 1]
        else:
            parts = total.reshape(planes, rows, 2 * wide)
            low, high = parts[:, :, :wide], parts[:, :, wide:]

        @pl.when(core == 0)
        def _():
            mine[:, k] = low
            theirs[:, k] = high.astype(BF16)

        @pl.when(core == 1)
        def _():
            mine[:, k] = high
            theirs[:, k] = low.astype(BF16)

        return carry

    lax.fori_loop(0, count * bonds, pick, 0)
    lax.fori_loop(0, count, one, 0)


def product(piece, start, sizes, place, sources, env, waves=None, count_all=None):
    own, count, width, _ = env[0].shape
    lanes = width // 2
    second = waves is not None
    lines = sources[0].shape[0] // 2
    planes = GRID[0]
    rows, columns = (width // planes // 2, width) if second else (width // planes, lanes)
    shape = (planes, count, rows, columns)
    picked = (count * 2 * own, width, lanes)
    out_shape = [jax.ShapeDtypeStruct(shape, F32), jax.ShapeDtypeStruct(shape, BF16)]
    if not second:
        out_shape.append(jax.ShapeDtypeStruct(picked, BF16))
    operands = list(sources) + ([waves] if second else []) + list(env)
    return pl.pallas_call(
        functools.partial(product_kernel, second, count_all, lines),
        in_specs=[pl.BlockSpec(memory_space=pltpu.SMEM)] * 4 + [pl.BlockSpec(memory_space=pltpu.VMEM)] * len(operands),
        out_specs=[pl.BlockSpec(memory_space=pltpu.VMEM)] * len(out_shape),
        scratch_shapes=[pltpu.VMEM(picked, BF16)] if second else [],
        out_shape=out_shape,
        compiler_params=pltpu.CompilerParams(vmem_limit_bytes=16 << 20),
        name="product",
    )(piece, start, sizes, place, *operands)


def along_z(mine, theirs):
    both = (mine + swapped(theirs).astype(F32)).astype(BF16)
    return lax.all_to_all(both, "z", split_axis=0, concat_axis=0, tiled=True)


def body(wavefunction, left_env, right_env, source, block_size):
    count, width, _ = wavefunction.shape
    lanes = width // 2
    z, core = lax.axis_index("z"), lax.axis_index("core")
    sector = lax.axis_index("y") * RING + lax.axis_index("x")
    place = jnp.stack([z, core]).astype(jnp.int32)
    waves = plane_gather(masked_half(core, block_size, wavefunction))

    own_source = lax.dynamic_slice_in_dim(source, sector * count, count, 1)
    needs = jnp.concatenate([own_source, swapped(own_source)], axis=0).T.reshape(-1)
    left_other = swapped(left_env)
    right_other = swapped(lax.dynamic_slice_in_dim(right_env, (1 - core) * lanes, lanes, 3))
    env = (left_env, left_other, right_env, right_other)

    piece, start = places_of(needs, count * width, count, width)
    mine, theirs, picked = product(piece, start, block_size, place, waves, env)
    first, message = middle(place, block_size, along_z(mine, theirs), wavefunction)

    gathered = lax.all_gather(message, ("z", "core"), axis=0, tiled=False)
    firsts = plane_gather(collect(place, gathered, count))
    rows = width // GRID[0] // 2
    kept = lax.dynamic_slice_in_dim(first, core * rows, rows, 1)
    given = swapped(lax.dynamic_slice_in_dim(first, (1 - core) * rows, rows, 1))
    low, high = jnp.where(core == 0, kept, given), jnp.where(core == 0, given, kept)
    first_product = jnp.concatenate([low, high], axis=2)

    piece, start = places_of(needs, count * width + EXTRA, count, width)
    count_all = RING * RING * count * width * width
    mine, theirs = product(piece, start, block_size, place, firsts, env, picked, count_all)
    second_product = jnp.sum(along_z(mine, theirs).astype(F32), axis=0)
    return (first_product, second_product)


def solution(mesh):
    chips = Mesh(mesh.devices.reshape(GRID), AXES)
    term, sector = ("z", "core"), ("y", "x")
    placed = (
        P(sector, None, None),
        P(term, sector, None, None),
        P(term, sector, None, None),
        P(term, None),
        P(sector, None),
    )
    return jax.shard_map(
        body,
        mesh=chips,
        in_specs=placed,
        out_specs=(P(sector, term, None), P(sector, term, None)),
        check_vma=False,
    )
```

```python
import functools

import jax
import jax.numpy as jnp
from jax import lax
from jax.experimental import pallas as pl
from jax.experimental.pallas import tpu as pltpu
from jax.sharding import Mesh, PartitionSpec as P

epsilon = 1e-06
AXES = ("z", "core", "y", "x")
GRID = (8, 2, 4, 4)
RING = 4
EXTRA = 16
F32 = jnp.float32
BF16 = jnp.bfloat16


def pieces_of(value):
    pieces, rest = [], value
    for _ in range(3):
        piece = rest.astype(BF16)
        pieces.append(piece.astype(F32))
        rest = rest - pieces[-1]
    return pieces


def ratio(above, below):
    live = below > 0
    return jnp.where(live, above / jnp.where(live, below, 1.0), 0.0)


def totals_of(extra):
    parts = extra.astype(F32)
    norms = parts[:, 0] + parts[:, 1] + parts[:, 2]
    margins = parts[:, 3] + parts[:, 4] + parts[:, 5]
    spreads = parts[:, 6] + parts[:, 7] + parts[:, 8]
    norm = jnp.sum(norms, axis=0, keepdims=True)
    margin = jnp.sum(margins, axis=0, keepdims=True)
    own = ratio(margins, norms)
    shift = ratio(margin, norm) - own
    moved = spreads - 2.0 * shift * (margins - own * norms) + shift * shift * norms
    return norm, margin, jnp.sum(moved, axis=0, keepdims=True)


def rows_of_pieces(values, lanes):
    rows = [jnp.broadcast_to(row, (1, lanes)) for value in values for row in pieces_of(value)]
    rows.append(jnp.zeros((EXTRA - len(rows), lanes), F32))
    return jnp.concatenate(rows, axis=0).astype(BF16)


def keep_of(rows, columns, shape, first_row=0, first_column=0):
    row = lax.broadcasted_iota(jnp.int32, shape, 0) + first_row
    column = lax.broadcasted_iota(jnp.int32, shape, 1) + first_column
    return (row < rows) & (column < columns)


def masked_half(core, sizes, wave):
    count, width, _ = wave.shape
    lanes = width // 2
    part = lax.dynamic_slice_in_dim(wave, core * lanes, lanes, 2)
    row = lax.broadcasted_iota(jnp.int32, part.shape, 1)
    column = lax.broadcasted_iota(jnp.int32, part.shape, 2) + core * lanes
    keep = (row < sizes[0][:, None, None]) & (column < sizes[1][:, None, None])
    return jnp.where(keep, part, jnp.zeros_like(part)).reshape(count * width, lanes)


def middle_kernel(place, sizes, arrived, wave, first_out, message):
    peers, count, rows, lanes = arrived.shape
    summed = arrived[0].astype(F32)
    for t in range(1, peers):
        summed = summed + arrived[t].astype(F32)
    first_out[...] = summed
    kept = []
    for k in range(count):
        keep = keep_of(sizes[0, k], sizes[1, k], (rows, lanes), place[0] * rows, place[1] * lanes)
        kept.append(jnp.where(keep, wave[k].astype(F32), 0.0)[None])
    masked = jnp.concatenate(kept, axis=0)

    def whole(values):
        return jnp.sum(jnp.sum(jnp.sum(values, axis=0), axis=0, keepdims=True), axis=1, keepdims=True)

    margin = whole(masked * summed)
    norm = whole(masked * masked)
    residual = summed - ratio(margin, norm)[None] * masked
    spread = whole(residual * residual)
    message[pl.ds(0, count * rows), :] = summed.astype(BF16).reshape(count * rows, lanes)
    message[pl.ds(count * rows, EXTRA), :] = rows_of_pieces((norm, margin, spread), lanes)


def middle(place, sizes, arrived, wave):
    peers, count, rows, lanes = arrived.shape
    lines = count * rows + EXTRA
    return pl.pallas_call(
        middle_kernel,
        grid_spec=pltpu.PrefetchScalarGridSpec(
            num_scalar_prefetch=2,
            grid=(1,),
            in_specs=[
                pl.BlockSpec((peers, count, rows, lanes), lambda i, *_: (0, 0, 0, 0)),
                pl.BlockSpec((count, rows, lanes), lambda i, place, *_: (0, place[0], place[1])),
            ],
            out_specs=[
                pl.BlockSpec((count, rows, lanes), lambda i, *_: (0, 0, 0)),
                pl.BlockSpec((lines, lanes), lambda i, *_: (0, 0)),
            ],
        ),
        out_shape=[
            jax.ShapeDtypeStruct((count, rows, lanes), F32),
            jax.ShapeDtypeStruct((lines, lanes), BF16),
        ],
        compiler_params=pltpu.CompilerParams(vmem_limit_bytes=8 << 20),
        name="middle",
    )(place, sizes, arrived, wave)


def collect_kernel(count, place, gathered, out):
    terms, lines, lanes = gathered.shape
    rows = (lines - EXTRA) // count
    planes = terms // 2
    width = planes * rows
    for z in range(planes):
        part = gathered[2 * z + place[1]]
        for k in range(count):
            out[pl.ds(k * width + z * rows, rows), :] = part[k * rows : (k + 1) * rows]
    totals = totals_of(gathered[:, pl.ds(count * rows, EXTRA), :])
    out[pl.ds(count * width, EXTRA), :] = rows_of_pieces(totals, lanes)


def collect(place, gathered, count):
    terms, lines, lanes = gathered.shape
    out_lines = terms // 2 * (lines - EXTRA) + EXTRA
    return pl.pallas_call(
        functools.partial(collect_kernel, count),
        grid_spec=pltpu.PrefetchScalarGridSpec(
            num_scalar_prefetch=1,
            grid=(1,),
            in_specs=[pl.BlockSpec((terms, lines, lanes), lambda i, *_: (0, 0, 0))],
            out_specs=pl.BlockSpec((out_lines, lanes), lambda i, *_: (0, 0)),
        ),
        out_shape=jax.ShapeDtypeStruct((out_lines, lanes), BF16),
        compiler_params=pltpu.CompilerParams(vmem_limit_bytes=8 << 20),
        name="collect",
    )(place, gathered)


def plane_pairs(inner, distance):
    pairs = []
    for core in range(2):
        for y in range(RING):
            for x in range(RING):
                if (core == 0) == inner:
                    to = (y, (x + distance) % RING)
                else:
                    to = ((y + distance) % RING, x)
                pairs.append(((core * RING + y) * RING + x, (core * RING + to[0]) * RING + to[1]))
    return pairs


def moved(array, inner, distance):
    return lax.ppermute(array, ("core", "y", "x"), plane_pairs(inner, distance))


def swapped(array):
    return lax.ppermute(array, "core", [(0, 1), (1, 0)])


def plane_gather(own):
    low = jnp.concatenate([own, moved(own, True, 1)], axis=0)
    high = jnp.concatenate([moved(own, True, -1), moved(own, True, 2)], axis=0)
    below_low, above_high = moved(low, False, 1), moved(high, False, -1)
    below_high, above_low = moved(high, False, 1), moved(low, False, -1)
    far_low, far_high = moved(below_low, False, 1), moved(above_high, False, -1)
    return [low, high, above_low, above_high, far_low, far_high, below_low, below_high]


def place_of(owner, place):
    y_off = ((owner >> 2) - place[2]) & (RING - 1)
    x_off = (owner - place[3]) & (RING - 1)
    first = place[1] == 0
    inner = jnp.where(first, x_off, y_off)
    outer = jnp.where(first, y_off, x_off)
    order = jnp.where(inner == 0, 0, jnp.where(inner == 3, 1, inner + 1))
    return 2 * outer + (order >> 1), order & 1


def product_kernel(second, count_all, lines, source, source_other, sizes, place, *refs):
    sources, refs = refs[:8], refs[8:]
    if second:
        waves, left, left_other, right, right_other, mine, theirs, vectors = refs
    else:
        left, left_other, right, right_other, mine, theirs, vectors = refs
    own, count, width, _ = left.shape
    lanes = width // 2
    bonds = 2 * own
    core = place[1]
    columns = pl.ds(pl.multiple_of(core * lanes, lanes), lanes)
    if second:
        tails = [ref[pl.ds(slot * lines + lines - EXTRA, EXTRA), :][None] for ref in sources for slot in range(2)]
        norm, margin, spread = totals_of(jnp.concatenate(tails, axis=0))
        scale = lax.rsqrt(jnp.maximum(spread, 0.0) / count_all + epsilon)
        share = margin / norm

    def pick(k, carry):
        target = (place[2] * RING + place[3]) * count + k
        for b in range(bonds):
            need = source[b, target] if b < own else source_other[b - own, target]
            owner = lax.div(need, jnp.int32(count))
            piece, turn = place_of(owner, place)
            line = pl.multiple_of(turn * lines + (need - owner * count) * width, EXTRA)
            for n, ref in enumerate(sources):

                @pl.when(piece == n)
                def _():
                    vectors[k * bonds + b] = ref[pl.ds(line, width), :]

        return carry

    def one(k, carry):
        halves, rights = [], []
        for b in range(bonds):
            vector = vectors[k * bonds + b]
            if second:
                residual = vector.astype(F32) - share * waves[k * bonds + b].astype(F32)
                vector = (residual * scale).astype(BF16)
            at = b % own
            env = left if b < own else left_other
            halves.append(jnp.dot(env[at, k], vector, preferred_element_type=F32).astype(BF16))
            rights.append((right if b < own else right_other)[at, k, :, columns])
        total = lax.dot_general(
            jnp.concatenate(halves, axis=1),
            jnp.concatenate(rights, axis=1),
            (((1,), (1,)), ((), ())),
            preferred_element_type=F32,
        )
        total = jnp.where(keep_of(sizes[0, k], sizes[1, k], total.shape), total, 0.0)
        planes, _, rows, wide = mine.shape
        if second:
            parts = total.reshape(planes, 2, rows, wide)
            low, high = parts[:, 0], parts[:, 1]
        else:
            parts = total.reshape(planes, rows, 2 * wide)
            low, high = parts[:, :, :wide], parts[:, :, wide:]

        @pl.when(core == 0)
        def _():
            mine[:, k] = low
            theirs[:, k] = high.astype(BF16)

        @pl.when(core == 1)
        def _():
            mine[:, k] = high
            theirs[:, k] = low.astype(BF16)

        return carry

    lax.fori_loop(0, count, pick, 0)
    lax.fori_loop(0, count, one, 0)


def product(needs, sizes, place, sources, env, waves=None, count_all=None):
    own, count, width, _ = env[0].shape
    lanes = width // 2
    second = waves is not None
    lines = sources[0].shape[0] // 2
    planes = GRID[0]
    rows, columns = (width // planes // 2, width) if second else (width // planes, lanes)
    shape = (planes, count, rows, columns)
    picked = (count * 2 * own, width, lanes)
    out_shape = [jax.ShapeDtypeStruct(shape, F32), jax.ShapeDtypeStruct(shape, BF16)]
    if not second:
        out_shape.append(jax.ShapeDtypeStruct(picked, BF16))
    operands = list(sources) + ([waves] if second else []) + list(env)
    return pl.pallas_call(
        functools.partial(product_kernel, second, count_all, lines),
        in_specs=[pl.BlockSpec(memory_space=pltpu.SMEM)] * 4 + [pl.BlockSpec(memory_space=pltpu.VMEM)] * len(operands),
        out_specs=[pl.BlockSpec(memory_space=pltpu.VMEM)] * len(out_shape),
        scratch_shapes=[pltpu.VMEM(picked, BF16)] if second else [],
        out_shape=out_shape,
        compiler_params=pltpu.CompilerParams(vmem_limit_bytes=16 << 20),
        name="product",
    )(*needs, sizes, place, *operands)


def staged_kernel(*refs):
    count = len(refs) // 2
    copies = [pltpu.make_async_copy(refs[e], refs[count + e], refs[-1].at[e]) for e in range(count)]
    for copy in copies:
        copy.start()
    for copy in copies:
        copy.wait()


def staged(arrays):
    size = sum(array.size for array in arrays) * 2
    return pl.pallas_call(
        staged_kernel,
        in_specs=[pl.BlockSpec(memory_space=pl.ANY)] * len(arrays),
        out_specs=[pl.BlockSpec(memory_space=pltpu.VMEM)] * len(arrays),
        scratch_shapes=[pltpu.SemaphoreType.DMA((len(arrays),))],
        out_shape=[jax.ShapeDtypeStruct(array.shape, array.dtype) for array in arrays],
        compiler_params=pltpu.CompilerParams(vmem_limit_bytes=16 << 20),
        cost_estimate=pl.CostEstimate(flops=1 << 24, bytes_accessed=2 * size, transcendentals=0),
        name="staged",
    )(*arrays)


def along_z(mine, theirs):
    both = (mine + swapped(theirs).astype(F32)).astype(BF16)
    return lax.all_to_all(both, "z", split_axis=0, concat_axis=0, tiled=True)


def body(wavefunction, left_env, right_env, source, block_size):
    count, width, _ = wavefunction.shape
    lanes = width // 2
    core = lax.axis_index("core")
    place = jnp.stack([lax.axis_index(axis) for axis in AXES]).astype(jnp.int32)
    sizes = block_size.T
    waves = plane_gather(masked_half(core, sizes, wavefunction))
    needs = (source, swapped(source))
    left_other, right_other = staged([swapped(left_env), swapped(right_env)])
    env = (left_env, left_other, right_env, right_other)
    waves = [*staged(waves[:4]), *waves[4:6], *staged(waves[6:])]

    mine, theirs, picked = product(needs, sizes, place, waves, env)
    first, message = middle(place, sizes, along_z(mine, theirs), wavefunction)

    gathered = lax.all_gather(message, ("z", "core"), axis=0, tiled=False)
    firsts = plane_gather(collect(place, gathered, count))
    rows = width // GRID[0] // 2
    kept = lax.dynamic_slice_in_dim(first, core * rows, rows, 1)
    given = swapped(lax.dynamic_slice_in_dim(first, (1 - core) * rows, rows, 1))
    low, high = jnp.where(core == 0, kept, given), jnp.where(core == 0, given, kept)
    first_product = jnp.concatenate([low, high], axis=2)

    count_all = RING * RING * count * width * width
    mine, theirs = product(needs, sizes, place, firsts, env, picked, count_all)
    second_product = jnp.sum(along_z(mine, theirs).astype(F32), axis=0)
    return (first_product, second_product)


def solution(mesh):
    chips = Mesh(mesh.devices.reshape(GRID), AXES)
    term, sector = ("z", "core"), ("y", "x")
    placed = (
        P(sector, None, None),
        P(term, sector, None, None),
        P(term, sector, None, None),
        P(term, None),
        P(sector, None),
    )
    return jax.shard_map(
        body,
        mesh=chips,
        in_specs=placed,
        out_specs=(P(sector, term, None), P(sector, term, None)),
        check_vma=False,
    )
```

```python
import functools

import jax
import jax.numpy as jnp
from jax import lax
from jax.experimental import pallas as pl
from jax.experimental.pallas import tpu as pltpu
from jax.sharding import Mesh, PartitionSpec as P

epsilon = 1e-06
AXES = ("z", "core", "y", "x")
GRID = (8, 2, 4, 4)
RING = 4
EXTRA = 16
CHIP_CAP = 4
PACKED = (2, 4, 5, 7)
F32 = jnp.float32
BF16 = jnp.bfloat16


def pieces_of(value):
    pieces, rest = [], value
    for _ in range(3):
        piece = rest.astype(BF16)
        pieces.append(piece.astype(F32))
        rest = rest - pieces[-1]
    return pieces


def ratio(above, below):
    live = below > 0
    return jnp.where(live, above / jnp.where(live, below, 1.0), 0.0)


def totals_of(extra):
    parts = extra.astype(F32)
    norms = parts[:, 0] + parts[:, 1] + parts[:, 2]
    margins = parts[:, 3] + parts[:, 4] + parts[:, 5]
    spreads = parts[:, 6] + parts[:, 7] + parts[:, 8]
    norm = jnp.sum(norms, axis=0, keepdims=True)
    margin = jnp.sum(margins, axis=0, keepdims=True)
    own = ratio(margins, norms)
    shift = ratio(margin, norm) - own
    moved = spreads - 2.0 * shift * (margins - own * norms) + shift * shift * norms
    return norm, margin, jnp.sum(moved, axis=0, keepdims=True)


def rows_of_pieces(values, lanes):
    rows = [jnp.broadcast_to(row, (1, lanes)) for value in values for row in pieces_of(value)]
    rows.append(jnp.zeros((EXTRA - len(rows), lanes), F32))
    return jnp.concatenate(rows, axis=0).astype(BF16)


def keep_of(rows, columns, shape, first_row=0, first_column=0):
    row = lax.broadcasted_iota(jnp.int32, shape, 0) + first_row
    column = lax.broadcasted_iota(jnp.int32, shape, 1) + first_column
    return (row < rows) & (column < columns)


def masked_half(core, sizes, wave):
    count, width, _ = wave.shape
    lanes = width // 2
    part = lax.dynamic_slice_in_dim(wave, core * lanes, lanes, 2)
    row = lax.broadcasted_iota(jnp.int32, part.shape, 1)
    column = lax.broadcasted_iota(jnp.int32, part.shape, 2) + core * lanes
    keep = (row < sizes[0][:, None, None]) & (column < sizes[1][:, None, None])
    return jnp.where(keep, part, jnp.zeros_like(part)).reshape(count * width, lanes)


def middle_kernel(place, sizes, arrived, wave, first_out, message):
    peers, count, rows, lanes = arrived.shape
    summed = arrived[0].astype(F32)
    for t in range(1, peers):
        summed = summed + arrived[t].astype(F32)
    first_out[...] = summed
    kept = []
    for k in range(count):
        keep = keep_of(sizes[0, k], sizes[1, k], (rows, lanes), place[0] * rows, place[1] * lanes)
        kept.append(jnp.where(keep, wave[k].astype(F32), 0.0)[None])
    masked = jnp.concatenate(kept, axis=0)

    def whole(values):
        return jnp.sum(jnp.sum(jnp.sum(values, axis=0), axis=0, keepdims=True), axis=1, keepdims=True)

    margin = whole(masked * summed)
    norm = whole(masked * masked)
    residual = summed - ratio(margin, norm)[None] * masked
    spread = whole(residual * residual)
    message[pl.ds(0, count * rows), :] = summed.astype(BF16).reshape(count * rows, lanes)
    message[pl.ds(count * rows, EXTRA), :] = rows_of_pieces((norm, margin, spread), lanes)


def middle(place, sizes, arrived, wave):
    peers, count, rows, lanes = arrived.shape
    lines = count * rows + EXTRA
    return pl.pallas_call(
        middle_kernel,
        grid_spec=pltpu.PrefetchScalarGridSpec(
            num_scalar_prefetch=2,
            grid=(1,),
            in_specs=[
                pl.BlockSpec((peers, count, rows, lanes), lambda i, *_: (0, 0, 0, 0)),
                pl.BlockSpec((count, rows, lanes), lambda i, place, *_: (0, place[0], place[1])),
            ],
            out_specs=[
                pl.BlockSpec((count, rows, lanes), lambda i, *_: (0, 0, 0)),
                pl.BlockSpec((lines, lanes), lambda i, *_: (0, 0)),
            ],
        ),
        out_shape=[
            jax.ShapeDtypeStruct((count, rows, lanes), F32),
            jax.ShapeDtypeStruct((lines, lanes), BF16),
        ],
        compiler_params=pltpu.CompilerParams(vmem_limit_bytes=8 << 20),
        name="middle",
    )(place, sizes, arrived, wave)


def collect_kernel(count, place, gathered, out):
    terms, lines, lanes = gathered.shape
    rows = (lines - EXTRA) // count
    planes = terms // 2
    width = planes * rows
    for z in range(planes):
        part = gathered[2 * z + place[1]]
        for k in range(count):
            out[pl.ds(k * width + z * rows, rows), :] = part[k * rows : (k + 1) * rows]
    totals = totals_of(gathered[:, pl.ds(count * rows, EXTRA), :])
    out[pl.ds(count * width, EXTRA), :] = rows_of_pieces(totals, lanes)


def collect(place, gathered, count):
    terms, lines, lanes = gathered.shape
    out_lines = terms // 2 * (lines - EXTRA) + EXTRA
    return pl.pallas_call(
        functools.partial(collect_kernel, count),
        grid_spec=pltpu.PrefetchScalarGridSpec(
            num_scalar_prefetch=1,
            grid=(1,),
            in_specs=[pl.BlockSpec((terms, lines, lanes), lambda i, *_: (0, 0, 0))],
            out_specs=pl.BlockSpec((out_lines, lanes), lambda i, *_: (0, 0)),
        ),
        out_shape=jax.ShapeDtypeStruct((out_lines, lanes), BF16),
        compiler_params=pltpu.CompilerParams(vmem_limit_bytes=8 << 20),
        name="collect",
    )(place, gathered)


def plane_pairs(inner, distance):
    pairs = []
    for core in range(2):
        for y in range(RING):
            for x in range(RING):
                if (core == 0) == inner:
                    to = (y, (x + distance) % RING)
                else:
                    to = ((y + distance) % RING, x)
                pairs.append(((core * RING + y) * RING + x, (core * RING + to[0]) * RING + to[1]))
    return pairs


def moved(array, inner, distance):
    return lax.ppermute(array, ("core", "y", "x"), plane_pairs(inner, distance))


def swapped(array):
    return lax.ppermute(array, "core", [(0, 1), (1, 0)])


def plane_gather(own, needs, place, width):
    low = jnp.concatenate([own, moved(own, True, 1)], axis=0)
    high = jnp.concatenate([moved(own, True, -1), moved(own, True, 2)], axis=0)
    below_low, above_high = moved(low, False, 1), moved(high, False, -1)
    below_high = moved(packed(high, 1, 0, 1, needs, place, width), False, 1)
    above_low = moved(packed(low, 0, 0, -1, needs, place, width), False, -1)
    far_low = moved(packed(below_low, 0, -1, 1, needs, place, width), False, 1)
    far_high = moved(packed(above_high, 1, 1, -1, needs, place, width), False, -1)
    return [low, high, above_low, above_high, far_low, far_high, below_low, below_high]


def packed_kernel(width, half, row, to, source, source_other, place, array, out, taken):
    own = source.shape[0]
    lines, kept = array.shape[0] // 2, out.shape[0] // 2
    tail = kept - CHIP_CAP * width
    count = (lines - tail) // width
    first = place[1] == 0
    inner = jnp.where(first, place[3], place[2])
    outer = jnp.where(first, place[2], place[3])

    def sector(inner_at, outer_at):
        inner_at, outer_at = inner_at & (RING - 1), outer_at & (RING - 1)
        return jnp.where(first, outer_at * RING + inner_at, inner_at * RING + outer_at)

    owners = [sector(inner + offset, outer + row) for offset in ((1, 2) if half else (0, -1))]
    target = sector(inner, outer + to) * count
    for turn in range(2):
        taken[turn] = 0
        if tail:
            out[pl.ds(turn * kept + CHIP_CAP * width, tail), :] = array[pl.ds(turn * lines + count * width, tail), :]

    def take(k, carry):
        for b in range(2 * own):
            need = source[b, target + k] if b < own else source_other[b - own, target + k]
            owner = lax.div(need, jnp.int32(count))
            for turn in range(2):

                @pl.when(owner == owners[turn])
                def _():
                    at = taken[turn]
                    start = pl.multiple_of(turn * lines + (need - owner * count) * width, EXTRA)
                    to_line = pl.multiple_of(turn * kept + jnp.minimum(at, CHIP_CAP - 1) * width, EXTRA)
                    out[pl.ds(to_line, width), :] = array[pl.ds(start, width), :]
                    taken[turn] = at + 1

        return carry

    lax.fori_loop(0, count, take, 0)


def packed(array, half, row, to, needs, place, width):
    lines, lanes = array.shape[0] // 2, array.shape[1]
    tail = lines % width
    size = 2 * (CHIP_CAP * width + tail)
    return pl.pallas_call(
        functools.partial(packed_kernel, width, half, row, to),
        in_specs=[pl.BlockSpec(memory_space=pltpu.SMEM)] * 3 + [pl.BlockSpec(memory_space=pltpu.VMEM)],
        out_specs=pl.BlockSpec(memory_space=pltpu.VMEM),
        scratch_shapes=[pltpu.SMEM((2,), jnp.int32)],
        out_shape=jax.ShapeDtypeStruct((size, lanes), array.dtype),
        compiler_params=pltpu.CompilerParams(vmem_limit_bytes=4 << 20),
        cost_estimate=pl.CostEstimate(flops=1 << 22, bytes_accessed=4 * size * lanes, transcendentals=0),
        name="packed",
    )(*needs, place, array)


def place_of(owner, place):
    y_off = ((owner >> 2) - place[2]) & (RING - 1)
    x_off = (owner - place[3]) & (RING - 1)
    first = place[1] == 0
    inner = jnp.where(first, x_off, y_off)
    outer = jnp.where(first, y_off, x_off)
    order = jnp.where(inner == 0, 0, jnp.where(inner == 3, 1, inner + 1))
    return 2 * outer + (order >> 1), order & 1


def product_kernel(second, count_all, lines, source, source_other, sizes, place, *refs):
    sources, refs = refs[:8], refs[8:]
    if second:
        waves, left, left_other, right, right_other, mine, theirs, vectors, named = refs
    else:
        left, left_other, right, right_other, mine, theirs, vectors, named = refs
    own, count, width, _ = left.shape
    lanes = width // 2
    bonds = 2 * own
    core = place[1]
    columns = pl.ds(pl.multiple_of(core * lanes, lanes), lanes)
    if second:
        tails = []
        for ref in sources:
            size = ref.shape[0]
            tails += [ref[pl.ds(end - EXTRA, EXTRA), :][None] for end in (size // 2, size)]
        norm, margin, spread = totals_of(jnp.concatenate(tails, axis=0))
        scale = lax.rsqrt(jnp.maximum(spread, 0.0) / count_all + epsilon)
        share = margin / norm

    kept = sources[PACKED[0]].shape[0] // 2
    for owner in range(RING * RING):
        named[owner] = 0

    def pick(k, carry):
        target = (place[2] * RING + place[3]) * count + k
        for b in range(bonds):
            need = source[b, target] if b < own else source_other[b - own, target]
            owner = lax.div(need, jnp.int32(count))
            piece, turn = place_of(owner, place)
            rank = named[owner]
            named[owner] = rank + 1
            whole = turn * lines + (need - owner * count) * width
            part = turn * kept + jnp.minimum(rank, CHIP_CAP - 1) * width
            for n, ref in enumerate(sources):

                @pl.when(piece == n)
                def _():
                    line = pl.multiple_of(part if n in PACKED else whole, EXTRA)
                    vectors[k * bonds + b] = ref[pl.ds(line, width), :]

        return carry

    def one(k, carry):
        halves, rights = [], []
        for b in range(bonds):
            vector = vectors[k * bonds + b]
            if second:
                residual = vector.astype(F32) - share * waves[k * bonds + b].astype(F32)
                vector = (residual * scale).astype(BF16)
            at = b % own
            env = left if b < own else left_other
            halves.append(jnp.dot(env[at, k], vector, preferred_element_type=F32).astype(BF16))
            rights.append((right if b < own else right_other)[at, k, :, columns])
        total = lax.dot_general(
            jnp.concatenate(halves, axis=1),
            jnp.concatenate(rights, axis=1),
            (((1,), (1,)), ((), ())),
            preferred_element_type=F32,
        )
        total = jnp.where(keep_of(sizes[0, k], sizes[1, k], total.shape), total, 0.0)
        planes, _, rows, wide = mine.shape
        if second:
            parts = total.reshape(planes, 2, rows, wide)
            low, high = parts[:, 0], parts[:, 1]
        else:
            parts = total.reshape(planes, rows, 2 * wide)
            low, high = parts[:, :, :wide], parts[:, :, wide:]

        @pl.when(core == 0)
        def _():
            mine[:, k] = low
            theirs[:, k] = high.astype(BF16)

        @pl.when(core == 1)
        def _():
            mine[:, k] = high
            theirs[:, k] = low.astype(BF16)

        return carry

    lax.fori_loop(0, count, pick, 0)
    lax.fori_loop(0, count, one, 0)


def product(needs, sizes, place, sources, env, waves=None, count_all=None):
    own, count, width, _ = env[0].shape
    lanes = width // 2
    second = waves is not None
    lines = sources[0].shape[0] // 2
    planes = GRID[0]
    rows, columns = (width // planes // 2, width) if second else (width // planes, lanes)
    shape = (planes, count, rows, columns)
    picked = (count * 2 * own, width, lanes)
    out_shape = [jax.ShapeDtypeStruct(shape, F32), jax.ShapeDtypeStruct(shape, BF16)]
    if not second:
        out_shape.append(jax.ShapeDtypeStruct(picked, BF16))
    operands = list(sources) + ([waves] if second else []) + list(env)
    return pl.pallas_call(
        functools.partial(product_kernel, second, count_all, lines),
        in_specs=[pl.BlockSpec(memory_space=pltpu.SMEM)] * 4 + [pl.BlockSpec(memory_space=pltpu.VMEM)] * len(operands),
        out_specs=[pl.BlockSpec(memory_space=pltpu.VMEM)] * len(out_shape),
        scratch_shapes=([pltpu.VMEM(picked, BF16)] if second else []) + [pltpu.SMEM((RING * RING,), jnp.int32)],
        out_shape=out_shape,
        compiler_params=pltpu.CompilerParams(vmem_limit_bytes=16 << 20),
        name="product",
    )(*needs, sizes, place, *operands)


def staged_kernel(*refs):
    count = len(refs) // 2
    copies = [pltpu.make_async_copy(refs[e], refs[count + e], refs[-1].at[e]) for e in range(count)]
    for copy in copies:
        copy.start()
    for copy in copies:
        copy.wait()


def staged(arrays):
    size = sum(array.size for array in arrays) * 2
    return pl.pallas_call(
        staged_kernel,
        in_specs=[pl.BlockSpec(memory_space=pl.ANY)] * len(arrays),
        out_specs=[pl.BlockSpec(memory_space=pltpu.VMEM)] * len(arrays),
        scratch_shapes=[pltpu.SemaphoreType.DMA((len(arrays),))],
        out_shape=[jax.ShapeDtypeStruct(array.shape, array.dtype) for array in arrays],
        compiler_params=pltpu.CompilerParams(vmem_limit_bytes=16 << 20),
        cost_estimate=pl.CostEstimate(flops=1 << 24, bytes_accessed=2 * size, transcendentals=0),
        name="staged",
    )(*arrays)


def along_z(mine, theirs):
    both = (mine + swapped(theirs).astype(F32)).astype(BF16)
    return lax.all_to_all(both, "z", split_axis=0, concat_axis=0, tiled=True)


def body(wavefunction, left_env, right_env, source, block_size):
    count, width, _ = wavefunction.shape
    lanes = width // 2
    core = lax.axis_index("core")
    place = jnp.stack([lax.axis_index(axis) for axis in AXES]).astype(jnp.int32)
    sizes = block_size.T
    needs = (source, swapped(source))
    waves = plane_gather(masked_half(core, sizes, wavefunction), needs, place, width)
    left_other, right_other = staged([swapped(left_env), swapped(right_env)])
    env = (left_env, left_other, right_env, right_other)
    waves = [*staged(waves[:4]), *waves[4:6], *staged(waves[6:])]

    mine, theirs, picked = product(needs, sizes, place, waves, env)
    first, message = middle(place, sizes, along_z(mine, theirs), wavefunction)

    gathered = lax.all_gather(message, ("z", "core"), axis=0, tiled=False)
    firsts = plane_gather(collect(place, gathered, count), needs, place, width)
    rows = width // GRID[0] // 2
    kept = lax.dynamic_slice_in_dim(first, core * rows, rows, 1)
    given = swapped(lax.dynamic_slice_in_dim(first, (1 - core) * rows, rows, 1))
    low, high = jnp.where(core == 0, kept, given), jnp.where(core == 0, given, kept)
    first_product = jnp.concatenate([low, high], axis=2)

    count_all = RING * RING * count * width * width
    mine, theirs = product(needs, sizes, place, firsts, env, picked, count_all)
    second_product = jnp.sum(along_z(mine, theirs).astype(F32), axis=0)
    return (first_product, second_product)


def solution(mesh):
    chips = Mesh(mesh.devices.reshape(GRID), AXES)
    term, sector = ("z", "core"), ("y", "x")
    placed = (
        P(sector, None, None),
        P(term, sector, None, None),
        P(term, sector, None, None),
        P(term, None),
        P(sector, None),
    )
    return jax.shard_map(
        body,
        mesh=chips,
        in_specs=placed,
        out_specs=(P(sector, term, None), P(sector, term, None)),
        check_vma=False,
    )
```

```python
import functools

import jax
import jax.numpy as jnp
from jax import lax
from jax.experimental import pallas as pl
from jax.experimental.pallas import tpu as pltpu
from jax.sharding import Mesh, PartitionSpec as P

epsilon = 1e-06
AXES = ("z", "core", "y", "x")
GRID = (8, 2, 4, 4)
RING = 4
EXTRA = 16
CHIP_CAP = 4
PACKED = (2, 4, 5, 7)
F32 = jnp.float32
BF16 = jnp.bfloat16


def pieces_of(value):
    pieces, rest = [], value
    for _ in range(3):
        piece = rest.astype(BF16)
        pieces.append(piece.astype(F32))
        rest = rest - pieces[-1]
    return pieces


def ratio(above, below):
    live = below > 0
    return jnp.where(live, above / jnp.where(live, below, 1.0), 0.0)


def totals_of(extra):
    parts = extra.astype(F32)
    norms = parts[:, 0] + parts[:, 1] + parts[:, 2]
    margins = parts[:, 3] + parts[:, 4] + parts[:, 5]
    spreads = parts[:, 6] + parts[:, 7] + parts[:, 8]
    norm = jnp.sum(norms, axis=0, keepdims=True)
    margin = jnp.sum(margins, axis=0, keepdims=True)
    own = ratio(margins, norms)
    shift = ratio(margin, norm) - own
    moved = spreads - 2.0 * shift * (margins - own * norms) + shift * shift * norms
    return norm, margin, jnp.sum(moved, axis=0, keepdims=True)


def rows_of_pieces(values, lanes):
    rows = [jnp.broadcast_to(row, (1, lanes)) for value in values for row in pieces_of(value)]
    rows.append(jnp.zeros((EXTRA - len(rows), lanes), F32))
    return jnp.concatenate(rows, axis=0).astype(BF16)


def keep_of(rows, columns, shape, first_row=0, first_column=0):
    row = lax.broadcasted_iota(jnp.int32, shape, 0) + first_row
    column = lax.broadcasted_iota(jnp.int32, shape, 1) + first_column
    return (row < rows) & (column < columns)


def masked_half(core, sizes, wave):
    count, width, _ = wave.shape
    lanes = width // 2
    part = lax.dynamic_slice_in_dim(wave, core * lanes, lanes, 2)
    row = lax.broadcasted_iota(jnp.int32, part.shape, 1)
    column = lax.broadcasted_iota(jnp.int32, part.shape, 2) + core * lanes
    keep = (row < sizes[0][:, None, None]) & (column < sizes[1][:, None, None])
    return jnp.where(keep, part, jnp.zeros_like(part)).reshape(count * width, lanes)


def middle_kernel(place, sizes, arrived, wave, first_out, message):
    peers, count, rows, lanes = arrived.shape
    summed = arrived[0].astype(F32)
    for t in range(1, peers):
        summed = summed + arrived[t].astype(F32)
    first_out[...] = summed
    kept = []
    for k in range(count):
        keep = keep_of(sizes[0, k], sizes[1, k], (rows, lanes), place[0] * rows, place[1] * lanes)
        kept.append(jnp.where(keep, wave[k].astype(F32), 0.0)[None])
    masked = jnp.concatenate(kept, axis=0)

    def whole(values):
        return jnp.sum(jnp.sum(jnp.sum(values, axis=0), axis=0, keepdims=True), axis=1, keepdims=True)

    margin = whole(masked * summed)
    norm = whole(masked * masked)
    residual = summed - ratio(margin, norm)[None] * masked
    spread = whole(residual * residual)
    message[pl.ds(0, count * rows), :] = summed.astype(BF16).reshape(count * rows, lanes)
    message[pl.ds(count * rows, EXTRA), :] = rows_of_pieces((norm, margin, spread), lanes)


def middle(place, sizes, arrived, wave):
    peers, count, rows, lanes = arrived.shape
    lines = count * rows + EXTRA
    return pl.pallas_call(
        middle_kernel,
        grid_spec=pltpu.PrefetchScalarGridSpec(
            num_scalar_prefetch=2,
            grid=(1,),
            in_specs=[
                pl.BlockSpec((peers, count, rows, lanes), lambda i, *_: (0, 0, 0, 0)),
                pl.BlockSpec((count, rows, lanes), lambda i, place, *_: (0, place[0], place[1])),
            ],
            out_specs=[
                pl.BlockSpec((count, rows, lanes), lambda i, *_: (0, 0, 0)),
                pl.BlockSpec((lines, lanes), lambda i, *_: (0, 0)),
            ],
        ),
        out_shape=[
            jax.ShapeDtypeStruct((count, rows, lanes), F32),
            jax.ShapeDtypeStruct((lines, lanes), BF16),
        ],
        compiler_params=pltpu.CompilerParams(vmem_limit_bytes=8 << 20),
        name="middle",
    )(place, sizes, arrived, wave)


def collect_kernel(count, place, gathered, out):
    terms, lines, lanes = gathered.shape
    rows = (lines - EXTRA) // count
    planes = terms // 2
    width = planes * rows
    for z in range(planes):
        part = gathered[2 * z + place[1]]
        for k in range(count):
            out[pl.ds(k * width + z * rows, rows), :] = part[k * rows : (k + 1) * rows]
    totals = totals_of(gathered[:, pl.ds(count * rows, EXTRA), :])
    out[pl.ds(count * width, EXTRA), :] = rows_of_pieces(totals, lanes)


def collect(place, gathered, count):
    terms, lines, lanes = gathered.shape
    out_lines = terms // 2 * (lines - EXTRA) + EXTRA
    return pl.pallas_call(
        functools.partial(collect_kernel, count),
        grid_spec=pltpu.PrefetchScalarGridSpec(
            num_scalar_prefetch=1,
            grid=(1,),
            in_specs=[pl.BlockSpec((terms, lines, lanes), lambda i, *_: (0, 0, 0))],
            out_specs=pl.BlockSpec((out_lines, lanes), lambda i, *_: (0, 0)),
        ),
        out_shape=jax.ShapeDtypeStruct((out_lines, lanes), BF16),
        compiler_params=pltpu.CompilerParams(vmem_limit_bytes=8 << 20),
        name="collect",
    )(place, gathered)


def plane_pairs(inner, distance):
    pairs = []
    for core in range(2):
        for y in range(RING):
            for x in range(RING):
                if (core == 0) == inner:
                    to = (y, (x + distance) % RING)
                else:
                    to = ((y + distance) % RING, x)
                pairs.append(((core * RING + y) * RING + x, (core * RING + to[0]) * RING + to[1]))
    return pairs


def moved(array, inner, distance):
    return lax.ppermute(array, ("core", "y", "x"), plane_pairs(inner, distance))


def swapped(array):
    return lax.ppermute(array, "core", [(0, 1), (1, 0)])


def plane_gather(own, needs, place, width):
    low = jnp.concatenate([own, moved(own, True, 1)], axis=0)
    high = jnp.concatenate([moved(own, True, -1), moved(own, True, 2)], axis=0)
    below_low, above_high = moved(low, False, 1), moved(high, False, -1)
    below_high = moved(packed(high, 1, 0, 1, needs, place, width), False, 1)
    above_low = moved(packed(low, 0, 0, -1, needs, place, width), False, -1)
    far_low = moved(packed(below_low, 0, -1, 1, needs, place, width), False, 1)
    far_high = moved(packed(above_high, 1, 1, -1, needs, place, width), False, -1)
    return [low, high, above_low, above_high, far_low, far_high, below_low, below_high]


def owner_of(sector, count):
    if count == 6:
        return (sector * 43) >> 8
    return lax.div(sector, jnp.int32(count))


def packed_kernel(width, half, row, to, source, source_other, place, array, out, taken):
    own = source.shape[0]
    lines, kept = array.shape[0] // 2, out.shape[0] // 2
    tail = kept - CHIP_CAP * width
    count = (lines - tail) // width
    first = place[1] == 0
    inner = jnp.where(first, place[3], place[2])
    outer = jnp.where(first, place[2], place[3])

    def sector(inner_at, outer_at):
        inner_at, outer_at = inner_at & (RING - 1), outer_at & (RING - 1)
        return jnp.where(first, outer_at * RING + inner_at, inner_at * RING + outer_at)

    owners = [sector(inner + offset, outer + row) for offset in ((1, 2) if half else (0, -1))]
    target = sector(inner, outer + to) * count
    for turn in range(2):
        taken[turn] = 0
        if tail:
            out[pl.ds(turn * kept + CHIP_CAP * width, tail), :] = array[pl.ds(turn * lines + count * width, tail), :]

    def take(k, carry):
        for b in range(2 * own):
            need = source[b, target + k] if b < own else source_other[b - own, target + k]
            owner = owner_of(need, count)
            for turn in range(2):

                @pl.when(owner == owners[turn])
                def _():
                    at = taken[turn]
                    start = pl.multiple_of(turn * lines + (need - owner * count) * width, EXTRA)
                    to_line = pl.multiple_of(turn * kept + jnp.minimum(at, CHIP_CAP - 1) * width, EXTRA)
                    out[pl.ds(to_line, width), :] = array[pl.ds(start, width), :]
                    taken[turn] = at + 1

        return carry

    lax.fori_loop(0, count, take, 0)


def packed(array, half, row, to, needs, place, width):
    lines, lanes = array.shape[0] // 2, array.shape[1]
    tail = lines % width
    size = 2 * (CHIP_CAP * width + tail)
    return pl.pallas_call(
        functools.partial(packed_kernel, width, half, row, to),
        in_specs=[pl.BlockSpec(memory_space=pltpu.SMEM)] * 3 + [pl.BlockSpec(memory_space=pltpu.VMEM)],
        out_specs=pl.BlockSpec(memory_space=pltpu.VMEM),
        scratch_shapes=[pltpu.SMEM((2,), jnp.int32)],
        out_shape=jax.ShapeDtypeStruct((size, lanes), array.dtype),
        compiler_params=pltpu.CompilerParams(vmem_limit_bytes=4 << 20),
        cost_estimate=pl.CostEstimate(flops=1 << 22, bytes_accessed=4 * size * lanes, transcendentals=0),
        name="packed",
    )(*needs, place, array)


def place_of(owner, place):
    y_off = ((owner >> 2) - place[2]) & (RING - 1)
    x_off = (owner - place[3]) & (RING - 1)
    first = place[1] == 0
    inner = jnp.where(first, x_off, y_off)
    outer = jnp.where(first, y_off, x_off)
    order = jnp.where(inner == 0, 0, jnp.where(inner == 3, 1, inner + 1))
    return 2 * outer + (order >> 1), order & 1


def product_kernel(second, count_all, lines, source, source_other, sizes, place, *refs):
    sources, refs = refs[:8], refs[8:]
    if second:
        waves, left, left_other, right, right_other, mine, theirs, vectors, named = refs
    else:
        left, left_other, right, right_other, mine, theirs, vectors, named = refs
    own, count, width, _ = left.shape
    lanes = width // 2
    bonds = 2 * own
    core = place[1]
    columns = pl.ds(pl.multiple_of(core * lanes, lanes), lanes)
    if second:
        tails = []
        for ref in sources:
            size = ref.shape[0]
            tails += [ref[pl.ds(end - EXTRA, EXTRA), :][None] for end in (size // 2, size)]
        norm, margin, spread = totals_of(jnp.concatenate(tails, axis=0))
        scale = lax.rsqrt(jnp.maximum(spread, 0.0) / count_all + epsilon)
        share = margin / norm

    kept = sources[PACKED[0]].shape[0] // 2
    for owner in range(RING * RING):
        named[owner] = 0

    def pick(k, carry):
        target = (place[2] * RING + place[3]) * count + k
        for b in range(bonds):
            need = source[b, target] if b < own else source_other[b - own, target]
            owner = owner_of(need, count)
            piece, turn = place_of(owner, place)
            rank = named[owner]
            named[owner] = rank + 1
            whole = turn * lines + (need - owner * count) * width
            part = turn * kept + jnp.minimum(rank, CHIP_CAP - 1) * width
            for n, ref in enumerate(sources):

                @pl.when(piece == n)
                def _():
                    line = pl.multiple_of(part if n in PACKED else whole, EXTRA)
                    vectors[k * bonds + b] = ref[pl.ds(line, width), :]

        return carry

    def one(k, carry):
        halves, rights = [], []
        for b in range(bonds):
            vector = vectors[k * bonds + b]
            if second:
                residual = vector.astype(F32) - share * waves[k * bonds + b].astype(F32)
                vector = (residual * scale).astype(BF16)
            at = b % own
            env = left if b < own else left_other
            halves.append(jnp.dot(env[at, k], vector, preferred_element_type=F32).astype(BF16))
            rights.append((right if b < own else right_other)[at, k, :, columns])
        total = lax.dot_general(
            jnp.concatenate(halves, axis=1),
            jnp.concatenate(rights, axis=1),
            (((1,), (1,)), ((), ())),
            preferred_element_type=F32,
        )
        total = jnp.where(keep_of(sizes[0, k], sizes[1, k], total.shape), total, 0.0)
        planes, _, rows, wide = mine.shape
        if second:
            parts = total.reshape(planes, 2, rows, wide)
            low, high = parts[:, 0], parts[:, 1]
        else:
            parts = total.reshape(planes, rows, 2 * wide)
            low, high = parts[:, :, :wide], parts[:, :, wide:]

        @pl.when(core == 0)
        def _():
            mine[:, k] = low
            theirs[:, k] = high.astype(BF16)

        @pl.when(core == 1)
        def _():
            mine[:, k] = high
            theirs[:, k] = low.astype(BF16)

        return carry

    lax.fori_loop(0, count, pick, 0)
    lax.fori_loop(0, count, one, 0)


def product(needs, sizes, place, sources, env, waves=None, count_all=None):
    own, count, width, _ = env[0].shape
    lanes = width // 2
    second = waves is not None
    lines = sources[0].shape[0] // 2
    planes = GRID[0]
    rows, columns = (width // planes // 2, width) if second else (width // planes, lanes)
    shape = (planes, count, rows, columns)
    picked = (count * 2 * own, width, lanes)
    out_shape = [jax.ShapeDtypeStruct(shape, F32), jax.ShapeDtypeStruct(shape, BF16)]
    if not second:
        out_shape.append(jax.ShapeDtypeStruct(picked, BF16))
    operands = list(sources) + ([waves] if second else []) + list(env)
    return pl.pallas_call(
        functools.partial(product_kernel, second, count_all, lines),
        in_specs=[pl.BlockSpec(memory_space=pltpu.SMEM)] * 4 + [pl.BlockSpec(memory_space=pltpu.VMEM)] * len(operands),
        out_specs=[pl.BlockSpec(memory_space=pltpu.VMEM)] * len(out_shape),
        scratch_shapes=([pltpu.VMEM(picked, BF16)] if second else []) + [pltpu.SMEM((RING * RING,), jnp.int32)],
        out_shape=out_shape,
        compiler_params=pltpu.CompilerParams(vmem_limit_bytes=16 << 20),
        name="product",
    )(*needs, sizes, place, *operands)


def staged_kernel(*refs):
    count = len(refs) // 2
    copies = [pltpu.make_async_copy(refs[e], refs[count + e], refs[-1].at[e]) for e in range(count)]
    for copy in copies:
        copy.start()
    for copy in copies:
        copy.wait()


def staged(arrays):
    size = sum(array.size for array in arrays) * 2
    return pl.pallas_call(
        staged_kernel,
        in_specs=[pl.BlockSpec(memory_space=pl.ANY)] * len(arrays),
        out_specs=[pl.BlockSpec(memory_space=pltpu.VMEM)] * len(arrays),
        scratch_shapes=[pltpu.SemaphoreType.DMA((len(arrays),))],
        out_shape=[jax.ShapeDtypeStruct(array.shape, array.dtype) for array in arrays],
        compiler_params=pltpu.CompilerParams(vmem_limit_bytes=16 << 20),
        cost_estimate=pl.CostEstimate(flops=1 << 24, bytes_accessed=2 * size, transcendentals=0),
        name="staged",
    )(*arrays)


def along_z(mine, theirs):
    both = (mine + swapped(theirs).astype(F32)).astype(BF16)
    return lax.all_to_all(both, "z", split_axis=0, concat_axis=0, tiled=True)


def body(wavefunction, left_env, right_env, source, block_size):
    count, width, _ = wavefunction.shape
    lanes = width // 2
    core = lax.axis_index("core")
    place = jnp.stack([lax.axis_index(axis) for axis in AXES]).astype(jnp.int32)
    sizes = block_size.T
    needs = (source, swapped(source))
    waves = plane_gather(masked_half(core, sizes, wavefunction), needs, place, width)
    left_other, right_other = staged([swapped(left_env), swapped(right_env)])
    env = (left_env, left_other, right_env, right_other)
    waves = [*staged(waves[:4]), *waves[4:6], *staged(waves[6:])]

    mine, theirs, picked = product(needs, sizes, place, waves, env)
    first, message = middle(place, sizes, along_z(mine, theirs), wavefunction)

    gathered = lax.all_gather(message, ("z", "core"), axis=0, tiled=False)
    firsts = plane_gather(collect(place, gathered, count), needs, place, width)
    rows = width // GRID[0] // 2
    kept = lax.dynamic_slice_in_dim(first, core * rows, rows, 1)
    given = swapped(lax.dynamic_slice_in_dim(first, (1 - core) * rows, rows, 1))
    low, high = jnp.where(core == 0, kept, given), jnp.where(core == 0, given, kept)
    first_product = jnp.concatenate([low, high], axis=2)

    count_all = RING * RING * count * width * width
    mine, theirs = product(needs, sizes, place, firsts, env, picked, count_all)
    second_product = jnp.sum(along_z(mine, theirs).astype(F32), axis=0)
    return (first_product, second_product)


def solution(mesh):
    chips = Mesh(mesh.devices.reshape(GRID), AXES)
    term, sector = ("z", "core"), ("y", "x")
    placed = (
        P(sector, None, None),
        P(term, sector, None, None),
        P(term, sector, None, None),
        P(term, None),
        P(sector, None),
    )
    return jax.shard_map(
        body,
        mesh=chips,
        in_specs=placed,
        out_specs=(P(sector, term, None), P(sector, term, None)),
        check_vma=False,
    )
```
